32 devices in a mesh: groups: 2 (over x), expert: 16 (over z, y, core).
Axes of the slice: x: 2, y: 2, z: 4, core: 2. Of those that a mesh axis runs over, the one named last changes fastest.
Arguments:
- tokens: bfloat16 [512, 6144], P(('groups', 'expert')), parts along dimension 0, may hold values from -6 to 6
- route_ids: int32 [512, 2], P(('groups', 'expert')), parts along dimension 0, may hold values from 0 to 7, all different within a row; in each aligned block of 16 rows (0 to 15, 16 to 31, ...) at most 6 rows name the same one
- route_logits: float32 [512, 2], P(('groups', 'expert')), parts along dimension 0, may hold values from -6 to 6
- old_place: int32 [16], replicated, may hold values from 0 to 15, each once
- new_place: int32 [16], replicated, may hold values from 0 to 15, each once
- held_gate: bfloat16 [32, 6144, 128], P(('groups', 'expert')), parts along dimension 0, may hold values from -0.078125 to 0.078125
- held_up: bfloat16 [32, 6144, 128], P(('groups', 'expert')), parts along dimension 0, may hold values from -0.078125 to 0.078125
- held_down: bfloat16 [32, 6144, 128], P(('groups', 'expert')), parts along dimension 0, may hold values from -0.375 to 0.375
Outputs:
- moe_output: bfloat16 [512, 6144], P(('groups', 'expert')), parts along dimension 0
- moved_gate: bfloat16 [32, 6144, 128], P(('groups', 'expert')), parts along dimension 0
- moved_up: bfloat16 [32, 6144, 128], P(('groups', 'expert')), parts along dimension 0
- moved_down: bfloat16 [32, 6144, 128], P(('groups', 'expert')), parts along dimension 0
The draws below stay inside these ranges and needn't reach their ends.
There are 2 independent parts, one for each index of `groups`. The reference program is written for one: setup_inputs(seed, part) draws one part's arguments, and reference() takes and returns one part's arrays. A program takes and returns all parts, laid end to end along the dimension named above; an argument that names none is the same for every part. Nothing has to cross between parts.
Inputs may be any that keep to these rules, and one draw needn't show every extreme that they name: `route_ids`: within the rows of one device (aligned blocks of 16 rows) no expert is named by more than 6 rows, a bound that some block reaches; the two ids of a row differ. `old_place`: each device appears once. `new_place`: each device appears once.
All inputs are finite; a program needn't handle non-finite values.
Results may differ from the reference program's by a relative error of at most 0.0058.
Values may be sent and summed in bfloat16 or wider, within the bound.
A program may use at most 128 MiB of HBM per device.

```python
import math
import jax
import jax.numpy as jnp
import numpy as np
from jax import lax

D = 6144
F_SLOT = 128
EXPERTS = 8
TOP = 2
TOK_DEV = 16
CAP = 6
BLOCKS = 2
HIDDEN_SIZE = 256
TOKENS = 256
N_EXPERT = 16


def levels(stream_key, shape, pieces, low, top_value):
    gain, own = 1.0, jax.random.fold_in(stream_key, 6)
    for axis_at, shards_of in pieces:
        heights = jnp.exp(jax.random.uniform(jax.random.fold_in(own, axis_at), (shards_of,), jnp.float32, low / len(pieces), top_value / len(pieces)))
        gain = gain * jnp.repeat(heights, shape[axis_at] // shards_of).reshape([-1 if axis == axis_at else 1 for axis in range(len(shape))])
    return gain


def routed_block(key, own, number, rows, count, top, limit, slope):
    sequence = jax.random.permutation(key, count)
    heavy_load, usual = load_shares(count, rows * top, limit, slope, True), load_shares(count, rows * top, limit, slope, False)
    places = jnp.arange(count)

    def named(tallies, rotation):
        used = int((tallies > 0).sum())
        fixed = max(1, used // 4)
        shifted = fixed + (places - fixed + rotation * (used - fixed)) % max(1, count - fixed)
        return jnp.zeros((count,), jnp.int32).at[sequence[jnp.where(places < fixed, places, shifted)]].set(jnp.asarray(tallies, jnp.int32))

    tallies = jnp.where(number % 4 == 0, named(heavy_load, number // 4), named(usual, number - number // 4 - 1))
    mixed = jax.random.permutation(jax.random.fold_in(own, 3), count)
    giver, taker = mixed[0:count // 2 * 2:2], mixed[1:count // 2 * 2:2]
    room = jnp.minimum(tallies[giver] - 1, limit - tallies[taker]) // 2
    room = jnp.where((giver == sequence[0]) | (taker == sequence[0]) | (tallies[taker] == 0), 0, jnp.maximum(room, 0))
    shifted = jax.random.randint(jax.random.fold_in(own, 4), (count // 2,), 0, 1 << 20) % (room + 1)
    tallies = tallies.at[giver].add(-shifted).at[taker].add(shifted)
    items = jnp.searchsorted(jnp.cumsum(tallies), jnp.arange(rows * top), side="right").astype(jnp.int32)
    table = items.reshape(top, rows).T
    table = table[jax.random.permutation(jax.random.fold_in(own, 1), rows)]
    rotation = jax.random.randint(jax.random.fold_in(own, 2), (rows, 1), 0, top)
    return jnp.take_along_axis(table, (jnp.arange(top)[None, :] + rotation) % top, axis=1)


def load_shares(count, total, most, skew, full):
    loads = [(1 << 20) // math.isqrt(rank ** skew) + 1 for rank in range(1, count + 1)]
    largest = most if full else min(most, max(-(-total // count), total * loads[0] // sum(loads)))
    least = 1 if total - largest >= count - 1 else 0
    holding, spare = [largest] + [least] * (count - 1), total - largest - least * (count - 1)
    while spare > 0:
        movable = [i for i in range(1, count) if holding[i] < largest] or [i for i in range(1, count) if holding[i] < most]
        mass, left = sum([loads[i] for i in movable]), spare
        for i in movable:
            extra = min(most - holding[i], max(1, left * loads[i] // mass), spare)
            holding[i] = holding[i] + extra
            spare = spare - extra
    return np.array(holding)


def noise(stream_key, extent, spread, bound, pieces=(), kind=jnp.bfloat16):
    drawn = jax.random.normal(stream_key, extent, jnp.float32) * spread
    if len(pieces) > 0:
        drawn = levels(stream_key, extent, pieces, -0.22, 0.18) * drawn
    return jnp.clip(drawn, min=-bound, max=bound).astype(kind)


def setup_inputs(seed: int = 0, part: int = 0) -> dict:
    streams_of = jax.random.split(jax.random.key(seed), 9)
    part_keys = jax.random.split(jax.random.fold_in(streams_of[8], part), 9)
    tokens = noise(part_keys[0], (TOKENS, D), 1.0, 6.0, ((0, 16),))
    route_ids_keys = jax.random.split(jax.random.fold_in(part_keys[1], 1), TOKENS // TOK_DEV)
    route_ids_turns = jax.random.permutation(jax.random.fold_in(part_keys[1], 3), TOKENS // TOK_DEV)
    route_ids = jax.vmap(lambda own, number: routed_block(jax.random.fold_in(part_keys[1], 2), own, number, TOK_DEV, EXPERTS, TOP, CAP, 2))(route_ids_keys, route_ids_turns).reshape((TOKENS, TOP))
    route_logits = noise(part_keys[2], (TOKENS, TOP), 1.5, 6.0, ((0, 16),), jnp.float32)
    old_place = jax.random.permutation(streams_of[3], N_EXPERT).astype(jnp.int32)
    new_place = jax.random.permutation(streams_of[4], N_EXPERT).astype(jnp.int32)
    held_gate = noise(part_keys[5], (N_EXPERT, D, F_SLOT), D ** -0.5, 0.078125, ((0, 16),))
    held_up = noise(part_keys[6], (N_EXPERT, D, F_SLOT), D ** -0.5, 0.078125, ((0, 16),))
    held_down = noise(part_keys[7], (N_EXPERT, D, F_SLOT), HIDDEN_SIZE ** -0.5, 0.375, ((0, 16),))
    return dict(tokens=tokens, route_ids=route_ids, route_logits=route_logits, old_place=old_place, new_place=new_place, held_gate=held_gate, held_up=held_up, held_down=held_down)


def reference(tokens, route_ids, route_logits, old_place, new_place, held_gate, held_up, held_down):
    device_ids = jnp.arange(N_EXPERT, dtype=jnp.int32)
    slot_new_at = jnp.sum(jnp.where(new_place[:, None] == device_ids[None, :], device_ids[:, None], 0), axis=0).astype(jnp.int32)
    source_of = jnp.take(old_place, slot_new_at).astype(jnp.int32)
    moved_gate = jnp.take(held_gate, source_of, axis=0)
    moved_up = jnp.take(held_up, source_of, axis=0)
    moved_down = jnp.take(held_down, source_of, axis=0)
    first_weight = 1.0 / (1.0 + jnp.exp(route_logits[:, 1] - route_logits[:, 0]))
    second_weight = 1.0 / (1.0 + jnp.exp(route_logits[:, 0] - route_logits[:, 1]))
    weights = jnp.stack([first_weight, second_weight], axis=1).astype(jnp.float32)
    expert_ids = jnp.arange(EXPERTS, dtype=jnp.int32)
    route_hits = route_ids[:, :, None] == expert_ids[None, None, :]
    coefficient = jnp.sum(jnp.where(route_hits, weights[:, :, None], 0.0), axis=1).astype(jnp.float32)
    routed = jnp.any(route_hits, axis=1)

    def listing(column):
        return jnp.nonzero(column, size=N_EXPERT * CAP, fill_value=TOKENS)[0].astype(jnp.int32)

    index_table = jax.vmap(listing)(routed.T)
    padded_tokens = jnp.concatenate([tokens, jnp.zeros((1, D), jnp.bfloat16)], axis=0)
    padded_coeff = jnp.concatenate([coefficient, jnp.zeros((1, EXPERTS), jnp.float32)], axis=0)

    def apply_slot(slot_index, accumulated):
        expert_index = slot_index // BLOCKS
        row_index = jnp.take(index_table, expert_index, axis=0).astype(jnp.int32)
        slot_rows = jnp.take(padded_tokens, row_index, axis=0)
        holder = jnp.take(old_place, slot_index).astype(jnp.int32)
        w_gate = jnp.take(held_gate, holder, axis=0)
        w_up = jnp.take(held_up, holder, axis=0)
        w_down = jnp.take(held_down, holder, axis=0)
        gate_value = jnp.dot(slot_rows, w_gate, preferred_element_type=jnp.float32)
        up_value = jnp.dot(slot_rows, w_up, preferred_element_type=jnp.float32)
        hidden = (jax.nn.silu(gate_value) * up_value).astype(jnp.bfloat16)
        partial_value = jnp.dot(hidden, w_down.T, preferred_element_type=jnp.float32).astype(jnp.bfloat16)
        partial_value = lax.optimization_barrier(partial_value).astype(jnp.float32)
        scaling = jnp.take(padded_coeff, row_index, axis=0)[:, expert_index]
        return accumulated.at[row_index].add(scaling[:, None] * partial_value)

    start = jnp.zeros((TOKENS + 1, D), jnp.float32)
    summed = lax.fori_loop(0, N_EXPERT, apply_slot, start)
    moe_output = summed[:TOKENS].astype(jnp.bfloat16)
    return moe_output, moved_gate, moved_up, moved_down
```

```python
import functools

import jax
import jax.numpy as jnp
from jax import lax
from jax.experimental import pallas as pl
from jax.experimental.pallas import tpu as pltpu
from jax.sharding import PartitionSpec as P

EXPERTS = 8
LANES = 128
MESH = pl.DeviceIdType.MESH
VMEM_BYTES = 63_000_000


def layer_kernel(
    n,
    source_of,
    tok,
    coef,
    held_g,
    held_u,
    held_d,
    out,
    moved_g,
    moved_u,
    moved_d,
    tok_all,
    coef_all,
    w_gu,
    w_d,
    pieces_g,
    pieces_u,
    pieces_d,
    ordered,
    hidden,
    contrib,
    arrived,
    cross_out,
    cross_in,
    load_sem,
    tok_send,
    tok_recv,
    fwd_send,
    one_send,
    one_recv,
    two_send,
    two_recv,
    part_send,
    part_recv,
    cross_send,
    cross_recv,
):
    me = lax.axis_index("expert")
    half = n // 2
    base = (me // half) * half
    lane = me - base
    twin = lax.rem(me + half, n)
    twin_base = lax.rem(base + half, n)
    rows, width = tok.shape
    band = width // n
    held = (held_g, held_u, held_d)
    moved = (moved_g, moved_u, moved_d)
    pieces = (pieces_g, pieces_u, pieces_d)

    barrier = pltpu.get_barrier_semaphore()

    @pl.loop(1, n)
    def _(k):
        pl.semaphore_signal(
            barrier, inc=1, device_id={"expert": lax.rem(me + k, n)}, device_id_type=MESH
        )

    loads = (
        pltpu.make_async_copy(held_g.at[0], w_gu.at[:, pl.ds(0, LANES)], load_sem.at[0]),
        pltpu.make_async_copy(held_u.at[0], w_gu.at[:, pl.ds(LANES, LANES)], load_sem.at[1]),
        pltpu.make_async_copy(held_d.at[0], w_d, load_sem.at[2]),
    )
    for load in loads:
        load.start()

    def token_rows(owner):
        return pl.ds(pl.multiple_of(owner * rows, rows), rows)

    def band_rows(owner):
        return pl.ds(pl.multiple_of(owner * band, band), band)

    tok_all[token_rows(me), :] = tok[...]
    coef_all[token_rows(me), :] = coef[...]
    pl.semaphore_wait(barrier, n - 1)

    def token_copy(peer):
        return (
            pltpu.make_async_remote_copy(
                src_ref=tok, dst_ref=tok_all.at[token_rows(me)],
                send_sem=tok_send.at[0, peer], recv_sem=tok_recv.at[0, me],
                device_id={"expert": peer}, device_id_type=MESH,
            ),
            pltpu.make_async_remote_copy(
                src_ref=coef, dst_ref=coef_all.at[token_rows(me)],
                send_sem=tok_send.at[1, peer], recv_sem=tok_recv.at[1, me],
                device_id={"expert": peer}, device_id_type=MESH,
            ),
        )

    def twin_copy(peer):
        return (
            pltpu.make_async_remote_copy(
                src_ref=tok_all.at[token_rows(twin)], dst_ref=tok_all.at[token_rows(twin)],
                send_sem=fwd_send.at[0, peer], recv_sem=tok_recv.at[0, twin],
                device_id={"expert": peer}, device_id_type=MESH,
            ),
            pltpu.make_async_remote_copy(
                src_ref=coef_all.at[token_rows(twin)], dst_ref=coef_all.at[token_rows(twin)],
                send_sem=fwd_send.at[1, peer], recv_sem=tok_recv.at[1, twin],
                device_id={"expert": peer}, device_id_type=MESH,
            ),
        )

    def tokens_arrive(owner):
        pltpu.make_async_copy(tok, tok_all.at[token_rows(owner)], tok_recv.at[0, owner]).wait()
        pltpu.make_async_copy(coef, coef_all.at[token_rows(owner)], tok_recv.at[1, owner]).wait()

    def near(k):
        return base + lax.rem(lane + k, half)

    def band_copy(array, peer):
        return pltpu.make_async_remote_copy(
            src_ref=held[array].at[0, band_rows(peer)], dst_ref=pieces[array].at[me],
            send_sem=one_send.at[array], recv_sem=one_recv.at[array],
            device_id={"expert": peer}, device_id_type=MESH,
        )

    def spread(array):
        pltpu.make_async_copy(
            held[array].at[0, band_rows(me)], pieces[array].at[me], one_recv.at[array]
        ).start()

        @pl.loop(1, n)
        def _(k):
            band_copy(array, lax.rem(me + k, n)).start()

    def deliver(array):
        pltpu.make_async_copy(pieces[array], pieces[array], one_recv.at[array]).wait()

        @pl.loop(0, n)
        def _(slot):
            ordered[array, slot] = pieces[array][source_of[slot]]

        pltpu.make_async_copy(
            ordered.at[array, me], moved[array].at[0, band_rows(me)], two_recv.at[array]
        ).start()

        @pl.loop(1, n)
        def _(k):
            peer = lax.rem(me + k, n)
            pltpu.make_async_remote_copy(
                src_ref=ordered.at[array, peer], dst_ref=moved[array].at[0, band_rows(me)],
                send_sem=two_send.at[array], recv_sem=two_recv.at[array],
                device_id={"expert": peer}, device_id_type=MESH,
            ).start()

    for copy in token_copy(twin):
        copy.start()

    @pl.loop(1, half)
    def _(k):
        for copy in token_copy(near(k)):
            copy.start()

    spread(0)
    tokens_arrive(twin)

    @pl.loop(1, half)
    def _(k):
        for copy in twin_copy(near(k)):
            copy.start()

    spread(1)
    spread(2)

    @pl.loop(1, half)
    def _(k):
        tokens_arrive(near(k))
        tokens_arrive(twin_base + lax.rem(lane + k, half))

    for load in loads:
        load.wait()

    step = min(256, n * rows)
    columns = 512

    @pl.loop(0, n * rows // step)
    def _(block):
        at = pl.ds(pl.multiple_of(block * step, step), step)
        both = jnp.dot(tok_all[at, :], w_gu[...], preferred_element_type=jnp.float32)
        gate_value = both[:, :LANES]
        up_value = both[:, LANES:]
        hidden[...] = (gate_value / (1.0 + jnp.exp(-gate_value)) * up_value).astype(jnp.bfloat16)
        lanes = lax.broadcasted_iota(jnp.int32, (step, LANES), 1)
        scale = jnp.sum(jnp.where(lanes == me, coef_all[at, :], 0.0), axis=1, keepdims=True)

        @pl.loop(0, width // columns)
        def _(part):
            cols = pl.ds(pl.multiple_of(part * columns, columns), columns)
            value = lax.dot_general(
                hidden[...], w_d[cols, :], (((1,), (1,)), ((), ())),
                preferred_element_type=jnp.float32,
            )
            value = value.astype(jnp.bfloat16).astype(jnp.float32)
            contrib[at, cols] = (value * scale).astype(jnp.bfloat16)

    def part_copy(kind, peer):
        owner = peer if kind == 0 else lax.rem(peer + half, n)
        return pltpu.make_async_remote_copy(
            src_ref=contrib.at[token_rows(owner)], dst_ref=arrived.at[kind, lane],
            send_sem=part_send.at[kind, peer - base], recv_sem=part_recv.at[kind, lane],
            device_id={"expert": peer}, device_id_type=MESH,
        )

    for kind in (1, 0):

        @pl.loop(1, half)
        def _(k):
            part_copy(kind, near(k)).start()

    def add_up(kind, owner, extra, target):
        @pl.loop(1, half)
        def _(k):
            other = lax.rem(lane + k, half)
            pltpu.make_async_copy(
                arrived.at[kind, other], arrived.at[kind, other], part_recv.at[kind, other]
            ).wait()

        @pl.loop(0, width // columns)
        def _(part):
            cols = pl.ds(pl.multiple_of(part * columns, columns), columns)

            def more(k, total):
                return total + arrived[kind, lax.rem(lane + k, half), :, cols].astype(jnp.float32)

            total = contrib[token_rows(owner), cols].astype(jnp.float32)
            if extra is not None:
                total = total + extra[:, cols].astype(jnp.float32)
            target[:, cols] = lax.fori_loop(1, half, more, total).astype(jnp.bfloat16)

    deliver(0)
    add_up(1, twin, None, cross_out)
    cross = pltpu.make_async_remote_copy(
        src_ref=cross_out, dst_ref=cross_in, send_sem=cross_send, recv_sem=cross_recv,
        device_id={"expert": twin}, device_id_type=MESH,
    )
    cross.start()
    deliver(1)
    deliver(2)
    cross.wait()
    add_up(0, me, cross_in, out)

    for copy in token_copy(twin):
        copy.wait_send()

    @pl.loop(1, half)
    def _(k):
        for copy in token_copy(near(k)):
            copy.wait_send()
        for copy in twin_copy(near(k)):
            copy.wait_send()
        part_copy(0, near(k)).wait_send()
        part_copy(1, near(k)).wait_send()

    for array in range(3):
        most = pieces[array].at[pl.ds(0, n - 1)]
        pltpu.make_async_copy(most, most, one_send.at[array]).wait()
        pltpu.make_async_copy(most, most, two_send.at[array]).wait()
        pltpu.make_async_copy(
            moved[array].at[0], moved[array].at[0], two_recv.at[array]
        ).wait()


def per_device(
    tokens, route_ids, route_logits, old_place, new_place, held_gate, held_up, held_down
):
    n = lax.axis_size("expert")
    rows, width = tokens.shape
    band = width // n
    half = n // 2
    device_ids = jnp.arange(n, dtype=jnp.int32)
    blocks = n // EXPERTS
    at_new = (new_place[:, None] == device_ids[None, :]).astype(jnp.int32)
    at_old = (old_place[:, None] == device_ids[None, :]).astype(jnp.int32)
    source_of = jnp.sum(at_new * old_place[:, None], axis=0)
    expert_at = jnp.sum(at_old * device_ids[:, None], axis=0) // blocks
    first_weight = 1.0 / (1.0 + jnp.exp(route_logits[:, 1] - route_logits[:, 0]))
    second_weight = 1.0 / (1.0 + jnp.exp(route_logits[:, 0] - route_logits[:, 1]))
    coef = jnp.where(route_ids[:, 0:1] == expert_at[None, :], first_weight[:, None], 0.0)
    coef = coef + jnp.where(route_ids[:, 1:2] == expert_at[None, :], second_weight[:, None], 0.0)
    coef = jnp.pad(coef, ((0, 0), (0, LANES - n)))

    vmem = pl.BlockSpec(memory_space=pltpu.VMEM)
    anywhere = pl.BlockSpec(memory_space=pl.ANY)
    dma = pltpu.SemaphoreType.DMA
    moved_shape = jax.ShapeDtypeStruct(held_gate.shape, held_gate.dtype)
    return pl.pallas_call(
        functools.partial(layer_kernel, n),
        out_shape=(
            jax.ShapeDtypeStruct((rows, width), jnp.bfloat16),
            moved_shape,
            moved_shape,
            moved_shape,
        ),
        in_specs=[pl.BlockSpec(memory_space=pltpu.SMEM), vmem, vmem] + [anywhere] * 3,
        out_specs=(vmem, anywhere, anywhere, anywhere),
        scratch_shapes=[
            pltpu.VMEM((n * rows, width), jnp.bfloat16),
            pltpu.VMEM((n * rows, LANES), jnp.float32),
            pltpu.VMEM((width, 2 * LANES), jnp.bfloat16),
            pltpu.VMEM((width, LANES), jnp.bfloat16),
            pltpu.VMEM((n, band, LANES), jnp.bfloat16),
            pltpu.VMEM((n, band, LANES), jnp.bfloat16),
            pltpu.VMEM((n, band, LANES), jnp.bfloat16),
            pltpu.VMEM((3, n, band, LANES), jnp.bfloat16),
            pltpu.VMEM((min(256, n * rows), LANES), jnp.bfloat16),
            pltpu.VMEM((n * rows, width), jnp.bfloat16),
            pltpu.VMEM((2, half, rows, width), jnp.bfloat16),
            pltpu.VMEM((rows, width), jnp.bfloat16),
            pltpu.VMEM((rows, width), jnp.bfloat16),
            dma((3,)),
            dma((2, n)),
            dma((2, n)),
            dma((2, n)),
            dma((3,)),
            dma((3,)),
            dma((3,)),
            dma((3,)),
            dma((2, half)),
            dma((2, half)),
            dma,
            dma,
        ],
        compiler_params=pltpu.CompilerParams(
            collective_id=0, has_side_effects=True, vmem_limit_bytes=VMEM_BYTES
        ),
    )(source_of, tokens, coef, held_gate, held_up, held_down)


def solution(mesh):
    split = ("groups", "expert")
    placed = (
        P(split, None),
        P(split, None),
        P(split, None),
        P(),
        P(),
        P(split, None, None),
        P(split, None, None),
        P(split, None, None),
    )
    return jax.shard_map(
        per_device,
        mesh=mesh,
        in_specs=placed,
        out_specs=(
            P(split, None),
            P(split, None, None),
            P(split, None, None),
            P(split, None, None),
        ),
        check_vma=False,
    )
```

```python
import functools

import jax
import jax.numpy as jnp
from jax import lax
from jax.experimental import pallas as pl
from jax.experimental.pallas import tpu as pltpu
from jax.sharding import PartitionSpec as P

EXPERTS = 8
LANES = 128
MESH = pl.DeviceIdType.MESH
VMEM_BYTES = 63_000_000


def near_square_root(n):
    size = 1
    while size * size < n:
        size *= 2
    return size


def layer_kernel(
    n,
    most,
    table,
    tok,
    coef,
    held_g,
    held_u,
    held_d,
    out,
    moved_g,
    moved_u,
    moved_d,
    tok_all,
    coef_all,
    w_gu,
    w_d,
    pieces_g,
    pieces_u,
    pieces_d,
    crossed_g,
    crossed_u,
    crossed_d,
    ordered,
    hidden,
    contrib,
    part_in,
    plane_sum,
    half_in,
    cross_out,
    cross_in,
    load_sem,
    tok_send,
    fwd_send,
    plane_send,
    tok_recv,
    one_send,
    one_recv,
    two_send,
    two_recv,
    three_send,
    three_recv,
    part_send,
    part_recv,
    half_send,
    half_recv,
    cross_send,
    cross_recv,
):
    me = lax.axis_index("expert")
    half = n // 2
    base = (me // half) * half
    lane = me - base
    twin = lax.rem(me + half, n)
    rows, width = tok.shape
    band = width // half
    size = near_square_root(n)
    planes = n // size
    half_planes = planes // 2
    plane = me // size
    seat = me - plane * size
    my_plane_of_half = lane // size
    held = (held_g, held_u, held_d)
    moved = (moved_g, moved_u, moved_d)
    pieces = (pieces_g, pieces_u, pieces_d)
    crossed = (crossed_g, crossed_u, crossed_d)

    barrier = pltpu.get_barrier_semaphore()

    @pl.loop(1, n)
    def _(k):
        pl.semaphore_signal(
            barrier, inc=1, device_id={"expert": lax.rem(me + k, n)}, device_id_type=MESH
        )

    loads = (
        pltpu.make_async_copy(held_g.at[0], w_gu.at[:, pl.ds(0, LANES)], load_sem.at[0]),
        pltpu.make_async_copy(held_u.at[0], w_gu.at[:, pl.ds(LANES, LANES)], load_sem.at[1]),
        pltpu.make_async_copy(held_d.at[0], w_d, load_sem.at[2]),
    )
    for load in loads:
        load.start()

    def token_rows(owner):
        return pl.ds(pl.multiple_of(owner * rows, rows), rows)

    def band_rows(owner):
        return pl.ds(pl.multiple_of(owner * band, band), band)

    def near(k):
        return base + lax.rem(lane + k, half)

    def column(k):
        return base + lax.rem(lane + k * size, half)

    def mate(k):
        return plane * size + lax.rem(seat + k, size)

    def seated(other_plane):
        return other_plane * size + seat

    tok_all[token_rows(me), :] = tok[...]
    coef_all[token_rows(me), :] = coef[...]
    pl.semaphore_wait(barrier, n - 1)

    def send(source, target, send_sem, recv_sem, peer):
        return pltpu.make_async_remote_copy(
            src_ref=source, dst_ref=target, send_sem=send_sem, recv_sem=recv_sem,
            device_id={"expert": peer}, device_id_type=MESH,
        )

    def own_tokens(peer):
        at = token_rows(me)
        return (
            send(tok, tok_all.at[at], tok_send.at[0, peer], tok_recv.at[0, me], peer),
            send(coef, coef_all.at[at], tok_send.at[1, peer], tok_recv.at[1, me], peer),
        )

    def passed_tokens(owner, peer, sems):
        at = token_rows(owner)
        return (
            send(tok_all.at[at], tok_all.at[at], sems[0], tok_recv.at[0, owner], peer),
            send(coef_all.at[at], coef_all.at[at], sems[1], tok_recv.at[1, owner], peer),
        )

    def twin_tokens(peer):
        return passed_tokens(twin, peer, (fwd_send.at[0, peer], fwd_send.at[1, peer]))

    def plane_tokens(other_plane, k):
        sems = (plane_send.at[0, other_plane, k], plane_send.at[1, other_plane, k])
        return passed_tokens(seated(other_plane), mate(k), sems)

    def tokens_arrive(owner):
        pltpu.make_async_copy(tok, tok_all.at[token_rows(owner)], tok_recv.at[0, owner]).wait()
        pltpu.make_async_copy(coef, coef_all.at[token_rows(owner)], tok_recv.at[1, owner]).wait()

    def spread(array):
        pltpu.make_async_copy(
            held[array].at[0, band_rows(lane)], pieces[array].at[lane], one_recv.at[array]
        ).start()

        @pl.loop(1, half)
        def _(k):
            peer = near(k)
            send(
                held[array].at[0, band_rows(peer - base)], pieces[array].at[lane],
                one_send.at[array], one_recv.at[array], peer,
            ).start()

    def swap(array):
        return send(
            ordered.at[array, pl.ds(0, most)], crossed[array],
            two_send.at[array], two_recv.at[array], twin,
        )

    def cross_over(array):
        pltpu.make_async_copy(pieces[array], pieces[array], one_recv.at[array]).wait()

        @pl.loop(0, most)
        def _(m):
            ordered[array, m] = pieces[array][table[base + m]]

        swap(array).start()

    def deliver(array):
        swap(array).wait()

        @pl.loop(0, half)
        def _(place):
            at = base + place
            own = pieces[array][table[2 * n + at]]
            other = crossed[array][table[3 * n + at]]
            ordered[array, place] = jnp.where(table[n + at] == 1, other, own)

        pltpu.make_async_copy(
            ordered.at[array, lane], moved[array].at[0, band_rows(lane)], three_recv.at[array]
        ).start()

        @pl.loop(1, half)
        def _(k):
            peer = near(k)
            send(
                ordered.at[array, peer - base], moved[array].at[0, band_rows(lane)],
                three_send.at[array], three_recv.at[array], peer,
            ).start()

    for copy in own_tokens(twin):
        copy.start()

    @pl.loop(1, half_planes)
    def _(k):
        for copy in own_tokens(column(k)):
            copy.start()

    @pl.loop(1, size)
    def _(k):
        for copy in own_tokens(mate(k)):
            copy.start()

    spread(0)
    tokens_arrive(twin)

    @pl.loop(1, half_planes)
    def _(k):
        for copy in twin_tokens(column(k)):
            copy.start()

    spread(1)

    @pl.loop(1, half_planes)
    def _(k):
        tokens_arrive(column(k))
        tokens_arrive(lax.rem(column(k) + half, n))

    @pl.loop(1, planes)
    def _(shift):
        @pl.loop(1, size)
        def _(k):
            for copy in plane_tokens(lax.rem(plane + shift, planes), k):
                copy.start()

    spread(2)
    cross_over(0)

    @pl.loop(0, planes)
    def _(other_plane):
        @pl.loop(1, size)
        def _(k):
            tokens_arrive(other_plane * size + lax.rem(seat + k, size))

    for load in loads:
        load.wait()

    step = min(256, n * rows)
    columns = 512

    @pl.loop(0, n * rows // step)
    def _(block):
        at = pl.ds(pl.multiple_of(block * step, step), step)
        both = jnp.dot(tok_all[at, :], w_gu[...], preferred_element_type=jnp.float32)
        gate_value = both[:, :LANES]
        up_value = both[:, LANES:]
        hidden[...] = (gate_value / (1.0 + jnp.exp(-gate_value)) * up_value).astype(jnp.bfloat16)
        lanes = lax.broadcasted_iota(jnp.int32, (step, LANES), 1)
        scale = jnp.sum(jnp.where(lanes == me, coef_all[at, :], 0.0), axis=1, keepdims=True)

        @pl.loop(0, width // columns)
        def _(part):
            cols = pl.ds(pl.multiple_of(part * columns, columns), columns)
            value = lax.dot_general(
                hidden[...], w_d[cols, :], (((1,), (1,)), ((), ())),
                preferred_element_type=jnp.float32,
            )
            value = value.astype(jnp.bfloat16).astype(jnp.float32)
            contrib[at, cols] = (value * scale).astype(jnp.bfloat16)

    def part_copy(k, other_plane):
        peer = mate(k)
        owner = other_plane * size + lax.rem(seat + k, size)
        return send(
            contrib.at[token_rows(owner)], part_in.at[seat, other_plane],
            part_send.at[k, other_plane], part_recv.at[seat, other_plane], peer,
        )

    def half_copy(k, kind):
        peer = column(k)
        target = peer // size if kind == 0 else lax.rem(peer // size + half_planes, planes)
        return send(
            plane_sum.at[target], half_in.at[kind, my_plane_of_half],
            half_send.at[kind, k], half_recv.at[kind, my_plane_of_half], peer,
        )

    @pl.loop(0, planes)
    def _(other_plane):
        @pl.loop(1, size)
        def _(k):
            part_copy(k, other_plane).start()

    def add_plane():
        @pl.loop(0, planes)
        def _(other_plane):
            @pl.loop(1, size)
            def _(k):
                spot = part_in.at[lax.rem(seat + k, size), other_plane]
                pltpu.make_async_copy(
                    spot, spot, part_recv.at[lax.rem(seat + k, size), other_plane]
                ).wait()

            @pl.loop(0, width // columns)
            def _(part):
                cols = pl.ds(pl.multiple_of(part * columns, columns), columns)

                def more(k, total):
                    other = lax.rem(seat + k, size)
                    return total + part_in[other, other_plane, :, cols].astype(jnp.float32)

                total = contrib[token_rows(seated(other_plane)), cols].astype(jnp.float32)
                total = lax.fori_loop(1, size, more, total)
                plane_sum[other_plane, :, cols] = total.astype(jnp.bfloat16)

        for kind in (1, 0):

            @pl.loop(1, half_planes)
            def _(k):
                half_copy(k, kind).start()

    def add_half(kind, own_plane, extra, target):
        @pl.loop(1, half_planes)
        def _(k):
            other = lax.rem(my_plane_of_half + k, half_planes)
            spot = half_in.at[kind, other]
            pltpu.make_async_copy(spot, spot, half_recv.at[kind, other]).wait()

        @pl.loop(0, width // columns)
        def _(part):
            cols = pl.ds(pl.multiple_of(part * columns, columns), columns)

            def more(k, total):
                other = lax.rem(my_plane_of_half + k, half_planes)
                return total + half_in[kind, other, :, cols].astype(jnp.float32)

            total = plane_sum[own_plane, :, cols].astype(jnp.float32)
            if extra is not None:
                total = total + extra[:, cols].astype(jnp.float32)
            target[:, cols] = lax.fori_loop(1, half_planes, more, total).astype(jnp.bfloat16)

    cross_over(1)
    deliver(0)
    add_plane()
    cross_over(2)
    deliver(1)
    add_half(1, lax.rem(plane + half_planes, planes), None, cross_out)
    cross = send(cross_out, cross_in, cross_send, cross_recv, twin)
    cross.start()
    deliver(2)
    cross.wait()
    add_half(0, plane, cross_in, out)

    for copy in own_tokens(twin):
        copy.wait_send()

    @pl.loop(1, half_planes)
    def _(k):
        for copy in own_tokens(column(k)):
            copy.wait_send()
        for copy in twin_tokens(column(k)):
            copy.wait_send()
        half_copy(k, 0).wait_send()
        half_copy(k, 1).wait_send()

    @pl.loop(1, size)
    def _(k):
        for copy in own_tokens(mate(k)):
            copy.wait_send()

        @pl.loop(0, planes)
        def _(other_plane):
            part_copy(k, other_plane).wait_send()

        @pl.loop(1, planes)
        def _(shift):
            for copy in plane_tokens(lax.rem(plane + shift, planes), k):
                copy.wait_send()

    for array in range(3):
        sent = pieces[array].at[pl.ds(0, half - 1)]
        pltpu.make_async_copy(sent, sent, one_send.at[array]).wait()
        pltpu.make_async_copy(sent, sent, three_send.at[array]).wait()
        pltpu.make_async_copy(
            moved[array].at[0], moved[array].at[0], three_recv.at[array]
        ).wait()


def call_layer(n, most, which, table, tokens, coef, held_gate, held_up, held_down):
    rows, width = tokens.shape
    half = n // 2
    band = width // half
    size = near_square_root(n)
    planes = n // size
    vmem = pl.BlockSpec(memory_space=pltpu.VMEM)
    anywhere = pl.BlockSpec(memory_space=pl.ANY)
    dma = pltpu.SemaphoreType.DMA
    moved_shape = jax.ShapeDtypeStruct(held_gate.shape, held_gate.dtype)

    def block(*shape):
        return pltpu.VMEM(shape, jnp.bfloat16)

    return pl.pallas_call(
        functools.partial(layer_kernel, n, most),
        out_shape=(jax.ShapeDtypeStruct((rows, width), jnp.bfloat16),) + (moved_shape,) * 3,
        in_specs=[pl.BlockSpec(memory_space=pltpu.SMEM), vmem, vmem] + [anywhere] * 3,
        out_specs=(vmem, anywhere, anywhere, anywhere),
        scratch_shapes=[
            block(n * rows, width),
            pltpu.VMEM((n * rows, LANES), jnp.float32),
            block(width, 2 * LANES),
            block(width, LANES),
            block(half, band, LANES),
            block(half, band, LANES),
            block(half, band, LANES),
            block(most, band, LANES),
            block(most, band, LANES),
            block(most, band, LANES),
            block(3, half, band, LANES),
            block(min(256, n * rows), LANES),
            block(n * rows, width),
            block(size, planes, rows, width),
            block(planes, rows, width),
            block(2, planes // 2, rows, width),
            block(rows, width),
            block(rows, width),
            dma((3,)),
            dma((2, n)),
            dma((2, n)),
            dma((2, planes, size)),
            dma((2, n)),
            dma((3,)),
            dma((3,)),
            dma((3,)),
            dma((3,)),
            dma((3,)),
            dma((3,)),
            dma((size, planes)),
            dma((size, planes)),
            dma((2, planes // 2)),
            dma((2, planes // 2)),
            dma,
            dma,
        ],
        compiler_params=pltpu.CompilerParams(
            collective_id=which, has_side_effects=True, vmem_limit_bytes=VMEM_BYTES
        ),
    )(table, tokens, coef, held_gate, held_up, held_down)


def per_device(
    tokens, route_ids, route_logits, old_place, new_place, held_gate, held_up, held_down
):
    n = lax.axis_size("expert")
    half = n // 2
    device_ids = jnp.arange(n, dtype=jnp.int32)
    blocks = n // EXPERTS
    at_old = (old_place[:, None] == device_ids[None, :]).astype(jnp.int32)
    dest_of = jnp.sum(at_old * new_place[:, None], axis=0)
    expert_at = jnp.sum(at_old * device_ids[:, None], axis=0) // blocks
    half_of = device_ids // half
    crosses = (dest_of // half != half_of).astype(jnp.int32)
    earlier = (half_of[:, None] == half_of[None, :]) & (device_ids[:, None] < device_ids[None, :])
    turn = jnp.sum(earlier.astype(jnp.int32) * crosses[:, None], axis=0)
    lane_of = device_ids - half_of * half
    leaving = (half_of[:, None] * half + turn[:, None] == device_ids[None, :]).astype(jnp.int32)
    leaving = jnp.sum(leaving * (crosses * lane_of)[:, None], axis=0)
    arriving = (dest_of[:, None] == device_ids[None, :]).astype(jnp.int32)
    table = jnp.concatenate([
        leaving,
        jnp.sum(arriving * crosses[:, None], axis=0),
        jnp.sum(arriving * ((1 - crosses) * lane_of)[:, None], axis=0),
        jnp.sum(arriving * (crosses * turn)[:, None], axis=0),
    ])
    first_weight = 1.0 / (1.0 + jnp.exp(route_logits[:, 1] - route_logits[:, 0]))
    second_weight = 1.0 / (1.0 + jnp.exp(route_logits[:, 0] - route_logits[:, 1]))
    coef = jnp.where(route_ids[:, 0:1] == expert_at[None, :], first_weight[:, None], 0.0)
    coef = coef + jnp.where(route_ids[:, 1:2] == expert_at[None, :], second_weight[:, None], 0.0)
    coef = jnp.pad(coef, ((0, 0), (0, LANES - n)))
    levels = sorted({max(1, half * eighths // 8) for eighths in (3, 4, 5, 6, 8)})
    crossing = jnp.sum(crosses) // 2
    level = sum((crossing > most).astype(jnp.int32) for most in levels[:-1])
    branches = [functools.partial(call_layer, n, most, i) for i, most in enumerate(levels)]
    return lax.switch(level, branches, table, tokens, coef, held_gate, held_up, held_down)


def solution(mesh):
    split = ("groups", "expert")
    placed = (
        P(split, None),
        P(split, None),
        P(split, None),
        P(),
        P(),
        P(split, None, None),
        P(split, None, None),
        P(split, None, None),
    )
    return jax.shard_map(
        per_device,
        mesh=mesh,
        in_specs=placed,
        out_specs=(
            P(split, None),
            P(split, None, None),
            P(split, None, None),
            P(split, None, None),
        ),
        check_vma=False,
    )
```

```python
import functools

import jax
import jax.numpy as jnp
from jax import lax
from jax.experimental import pallas as pl
from jax.experimental.pallas import tpu as pltpu
from jax.sharding import PartitionSpec as P

EXPERTS = 8
LANES = 128
MESH = pl.DeviceIdType.MESH
VMEM_BYTES = 63_000_000


def near_square_root(n):
    size = 1
    while size * size < n:
        size *= 2
    return size


def layer_kernel(
    n,
    most,
    table,
    tok,
    coef,
    held_g,
    held_u,
    held_d,
    out,
    moved_g,
    moved_u,
    moved_d,
    tok_all,
    coef_all,
    w_gu,
    w_d,
    pieces_g,
    pieces_u,
    pieces_d,
    crossed_g,
    crossed_u,
    crossed_d,
    ordered,
    hidden,
    contrib,
    part_in,
    plane_sum,
    half_in,
    cross_out,
    cross_in,
    load_sem,
    tok_send,
    fwd_send,
    plane_send,
    tok_recv,
    one_send,
    one_recv,
    two_send,
    two_recv,
    three_send,
    three_recv,
    part_send,
    part_recv,
    half_send,
    half_recv,
    cross_send,
    cross_recv,
):
    me = lax.axis_index("expert")
    half = n // 2
    base = (me // half) * half
    lane = me - base
    twin = lax.rem(me + half, n)
    rows, width = tok.shape
    band = width // half
    size = near_square_root(n)
    planes = n // size
    half_planes = planes // 2
    plane = me // size
    seat = me - plane * size
    my_plane_of_half = lane // size
    held = (held_g, held_u, held_d)
    moved = (moved_g, moved_u, moved_d)
    pieces = (pieces_g, pieces_u, pieces_d)
    crossed = (crossed_g, crossed_u, crossed_d)

    barrier = pltpu.get_barrier_semaphore()

    @pl.loop(1, n)
    def _(k):
        pl.semaphore_signal(
            barrier, inc=1, device_id={"expert": lax.rem(me + k, n)}, device_id_type=MESH
        )

    loads = (
        pltpu.make_async_copy(held_g.at[0], w_gu.at[:, pl.ds(0, LANES)], load_sem.at[0]),
        pltpu.make_async_copy(held_u.at[0], w_gu.at[:, pl.ds(LANES, LANES)], load_sem.at[1]),
        pltpu.make_async_copy(held_d.at[0], w_d, load_sem.at[2]),
    )
    for load in loads:
        load.start()

    def token_rows(owner):
        return pl.ds(pl.multiple_of(owner * rows, rows), rows)

    def band_rows(owner):
        return pl.ds(pl.multiple_of(owner * band, band), band)

    def near(k):
        return base + lax.rem(lane + k, half)

    def column(k):
        return base + lax.rem(lane + k * size, half)

    def mate(k):
        return plane * size + lax.rem(seat + k, size)

    def seated(other_plane):
        return other_plane * size + seat

    tok_all[token_rows(me), :] = tok[...]
    coef_all[token_rows(me), :] = coef[...]
    pl.semaphore_wait(barrier, n - 1)

    def send(source, target, send_sem, recv_sem, peer):
        return pltpu.make_async_remote_copy(
            src_ref=source, dst_ref=target, send_sem=send_sem, recv_sem=recv_sem,
            device_id={"expert": peer}, device_id_type=MESH,
        )

    def own_tokens(peer):
        at = token_rows(me)
        return (
            send(tok, tok_all.at[at], tok_send.at[0, peer], tok_recv.at[0, me], peer),
            send(coef, coef_all.at[at], tok_send.at[1, peer], tok_recv.at[1, me], peer),
        )

    def passed_tokens(owner, peer, sems):
        at = token_rows(owner)
        return (
            send(tok_all.at[at], tok_all.at[at], sems[0], tok_recv.at[0, owner], peer),
            send(coef_all.at[at], coef_all.at[at], sems[1], tok_recv.at[1, owner], peer),
        )

    def twin_tokens(peer):
        return passed_tokens(twin, peer, (fwd_send.at[0, peer], fwd_send.at[1, peer]))

    def plane_tokens(other_plane, k):
        sems = (plane_send.at[0, other_plane, k], plane_send.at[1, other_plane, k])
        return passed_tokens(seated(other_plane), mate(k), sems)

    def tokens_arrive(owner):
        pltpu.make_async_copy(tok, tok_all.at[token_rows(owner)], tok_recv.at[0, owner]).wait()
        pltpu.make_async_copy(coef, coef_all.at[token_rows(owner)], tok_recv.at[1, owner]).wait()

    def spread(array):
        pltpu.make_async_copy(
            held[array].at[0, band_rows(lane)], pieces[array].at[lane], one_recv.at[array]
        ).start()

        @pl.loop(1, half)
        def _(k):
            peer = near(k)
            send(
                held[array].at[0, band_rows(peer - base)], pieces[array].at[lane],
                one_send.at[array], one_recv.at[array], peer,
            ).start()

    def swap(array):
        return send(
            ordered.at[array, pl.ds(0, most)], crossed[array],
            two_send.at[array], two_recv.at[array], twin,
        )

    def cross_over(array):
        pltpu.make_async_copy(pieces[array], pieces[array], one_recv.at[array]).wait()

        @pl.loop(0, most)
        def _(m):
            ordered[array, m] = pieces[array][table[base + m]]

        swap(array).start()

    def deliver(array):
        swap(array).wait()

        @pl.loop(0, half)
        def _(place):
            at = base + place
            own = pieces[array][table[2 * n + at]]
            other = crossed[array][table[3 * n + at]]
            ordered[array, place] = jnp.where(table[n + at] == 1, other, own)

        pltpu.make_async_copy(
            ordered.at[array, lane], moved[array].at[0, band_rows(lane)], three_recv.at[array]
        ).start()

        @pl.loop(1, half)
        def _(k):
            peer = near(k)
            send(
                ordered.at[array, peer - base], moved[array].at[0, band_rows(lane)],
                three_send.at[array], three_recv.at[array], peer,
            ).start()

    for copy in own_tokens(twin):
        copy.start()

    @pl.loop(1, half_planes)
    def _(k):
        for copy in own_tokens(column(k)):
            copy.start()

    @pl.loop(1, size)
    def _(k):
        for copy in own_tokens(mate(k)):
            copy.start()

    spread(0)
    tokens_arrive(twin)

    @pl.loop(1, half_planes)
    def _(k):
        for copy in twin_tokens(column(k)):
            copy.start()

    spread(1)

    @pl.loop(1, half_planes)
    def _(k):
        tokens_arrive(column(k))
        tokens_arrive(lax.rem(column(k) + half, n))

    @pl.loop(1, planes)
    def _(shift):
        @pl.loop(1, size)
        def _(k):
            for copy in plane_tokens(lax.rem(plane + shift, planes), k):
                copy.start()

    spread(2)
    cross_over(0)
    cross_over(1)

    @pl.loop(0, planes)
    def _(other_plane):
        @pl.loop(1, size)
        def _(k):
            tokens_arrive(other_plane * size + lax.rem(seat + k, size))

    for load in loads:
        load.wait()

    step = min(256, n * rows)
    columns = 512

    @pl.loop(0, n * rows // step)
    def _(block):
        at = pl.ds(pl.multiple_of(block * step, step), step)
        both = jnp.dot(tok_all[at, :], w_gu[...], preferred_element_type=jnp.float32)
        gate_value = both[:, :LANES]
        up_value = both[:, LANES:]
        hidden[...] = (gate_value / (1.0 + jnp.exp(-gate_value)) * up_value).astype(jnp.bfloat16)
        lanes = lax.broadcasted_iota(jnp.int32, (step, LANES), 1)
        scale = jnp.sum(jnp.where(lanes == me, coef_all[at, :], 0.0), axis=1, keepdims=True)

        @pl.loop(0, width // columns)
        def _(part):
            cols = pl.ds(pl.multiple_of(part * columns, columns), columns)
            value = lax.dot_general(
                hidden[...], w_d[cols, :], (((1,), (1,)), ((), ())),
                preferred_element_type=jnp.float32,
            )
            value = value.astype(jnp.bfloat16).astype(jnp.float32)
            contrib[at, cols] = (value * scale).astype(jnp.bfloat16)

    def part_copy(k, other_plane):
        peer = mate(k)
        owner = other_plane * size + lax.rem(seat + k, size)
        return send(
            contrib.at[token_rows(owner)], part_in.at[seat, other_plane],
            part_send.at[k, other_plane], part_recv.at[seat, other_plane], peer,
        )

    def half_copy(k, kind):
        peer = column(k)
        target = peer // size if kind == 0 else lax.rem(peer // size + half_planes, planes)
        return send(
            plane_sum.at[target], half_in.at[kind, my_plane_of_half],
            half_send.at[kind, k], half_recv.at[kind, my_plane_of_half], peer,
        )

    @pl.loop(0, planes)
    def _(other_plane):
        @pl.loop(1, size)
        def _(k):
            part_copy(k, other_plane).start()

    def add_plane():
        @pl.loop(0, planes)
        def _(other_plane):
            @pl.loop(1, size)
            def _(k):
                spot = part_in.at[lax.rem(seat + k, size), other_plane]
                pltpu.make_async_copy(
                    spot, spot, part_recv.at[lax.rem(seat + k, size), other_plane]
                ).wait()

            @pl.loop(0, width // columns)
            def _(part):
                cols = pl.ds(pl.multiple_of(part * columns, columns), columns)

                def more(k, total):
                    other = lax.rem(seat + k, size)
                    return total + part_in[other, other_plane, :, cols].astype(jnp.float32)

                total = contrib[token_rows(seated(other_plane)), cols].astype(jnp.float32)
                total = lax.fori_loop(1, size, more, total)
                plane_sum[other_plane, :, cols] = total.astype(jnp.bfloat16)

        for kind in (1, 0):

            @pl.loop(1, half_planes)
            def _(k):
                half_copy(k, kind).start()

    def add_half(kind, own_plane, extra, target):
        @pl.loop(1, half_planes)
        def _(k):
            other = lax.rem(my_plane_of_half + k, half_planes)
            spot = half_in.at[kind, other]
            pltpu.make_async_copy(spot, spot, half_recv.at[kind, other]).wait()

        @pl.loop(0, width // columns)
        def _(part):
            cols = pl.ds(pl.multiple_of(part * columns, columns), columns)

            def more(k, total):
                other = lax.rem(my_plane_of_half + k, half_planes)
                return total + half_in[kind, other, :, cols].astype(jnp.float32)

            total = plane_sum[own_plane, :, cols].astype(jnp.float32)
            if extra is not None:
                total = total + extra[:, cols].astype(jnp.float32)
            target[:, cols] = lax.fori_loop(1, half_planes, more, total).astype(jnp.bfloat16)

    deliver(0)
    cross_over(2)
    add_plane()
    deliver(1)
    add_half(1, lax.rem(plane + half_planes, planes), None, cross_out)
    cross = send(cross_out, cross_in, cross_send, cross_recv, twin)
    cross.start()
    deliver(2)
    cross.wait()
    add_half(0, plane, cross_in, out)

    for copy in own_tokens(twin):
        copy.wait_send()

    @pl.loop(1, half_planes)
    def _(k):
        for copy in own_tokens(column(k)):
            copy.wait_send()
        for copy in twin_tokens(column(k)):
            copy.wait_send()
        half_copy(k, 0).wait_send()
        half_copy(k, 1).wait_send()

    @pl.loop(1, size)
    def _(k):
        for copy in own_tokens(mate(k)):
            copy.wait_send()

        @pl.loop(0, planes)
        def _(other_plane):
            part_copy(k, other_plane).wait_send()

        @pl.loop(1, planes)
        def _(shift):
            for copy in plane_tokens(lax.rem(plane + shift, planes), k):
                copy.wait_send()

    for array in range(3):
        sent = pieces[array].at[pl.ds(0, half - 1)]
        pltpu.make_async_copy(sent, sent, one_send.at[array]).wait()
        pltpu.make_async_copy(sent, sent, three_send.at[array]).wait()
        pltpu.make_async_copy(
            moved[array].at[0], moved[array].at[0], three_recv.at[array]
        ).wait()


def call_layer(n, most, which, table, tokens, coef, held_gate, held_up, held_down):
    rows, width = tokens.shape
    half = n // 2
    band = width // half
    size = near_square_root(n)
    planes = n // size
    vmem = pl.BlockSpec(memory_space=pltpu.VMEM)
    anywhere = pl.BlockSpec(memory_space=pl.ANY)
    dma = pltpu.SemaphoreType.DMA
    moved_shape = jax.ShapeDtypeStruct(held_gate.shape, held_gate.dtype)

    def block(*shape):
        return pltpu.VMEM(shape, jnp.bfloat16)

    return pl.pallas_call(
        functools.partial(layer_kernel, n, most),
        out_shape=(jax.ShapeDtypeStruct((rows, width), jnp.bfloat16),) + (moved_shape,) * 3,
        in_specs=[pl.BlockSpec(memory_space=pltpu.SMEM), vmem, vmem] + [anywhere] * 3,
        out_specs=(vmem, anywhere, anywhere, anywhere),
        scratch_shapes=[
            block(n * rows, width),
            pltpu.VMEM((n * rows, LANES), jnp.float32),
            block(width, 2 * LANES),
            block(width, LANES),
            block(half, band, LANES),
            block(half, band, LANES),
            block(half, band, LANES),
            block(most, band, LANES),
            block(most, band, LANES),
            block(most, band, LANES),
            block(3, half, band, LANES),
            block(min(256, n * rows), LANES),
            block(n * rows, width),
            block(size, planes, rows, width),
            block(planes, rows, width),
            block(2, planes // 2, rows, width),
            block(rows, width),
            block(rows, width),
            dma((3,)),
            dma((2, n)),
            dma((2, n)),
            dma((2, planes, size)),
            dma((2, n)),
            dma((3,)),
            dma((3,)),
            dma((3,)),
            dma((3,)),
            dma((3,)),
            dma((3,)),
            dma((size, planes)),
            dma((size, planes)),
            dma((2, planes // 2)),
            dma((2, planes // 2)),
            dma,
            dma,
        ],
        compiler_params=pltpu.CompilerParams(
            collective_id=which, has_side_effects=True, vmem_limit_bytes=VMEM_BYTES
        ),
    )(table, tokens, coef, held_gate, held_up, held_down)


def per_device(
    tokens, route_ids, route_logits, old_place, new_place, held_gate, held_up, held_down
):
    n = lax.axis_size("expert")
    half = n // 2
    device_ids = jnp.arange(n, dtype=jnp.int32)
    blocks = n // EXPERTS
    at_old = (old_place[:, None] == device_ids[None, :]).astype(jnp.int32)
    dest_of = jnp.sum(at_old * new_place[:, None], axis=0)
    expert_at = jnp.sum(at_old * device_ids[:, None], axis=0) // blocks
    half_of = device_ids // half
    crosses = (dest_of // half != half_of).astype(jnp.int32)
    earlier = (half_of[:, None] == half_of[None, :]) & (device_ids[:, None] < device_ids[None, :])
    turn = jnp.sum(earlier.astype(jnp.int32) * crosses[:, None], axis=0)
    lane_of = device_ids - half_of * half
    leaving = (half_of[:, None] * half + turn[:, None] == device_ids[None, :]).astype(jnp.int32)
    leaving = jnp.sum(leaving * (crosses * lane_of)[:, None], axis=0)
    arriving = (dest_of[:, None] == device_ids[None, :]).astype(jnp.int32)
    table = jnp.concatenate([
        leaving,
        jnp.sum(arriving * crosses[:, None], axis=0),
        jnp.sum(arriving * ((1 - crosses) * lane_of)[:, None], axis=0),
        jnp.sum(arriving * (crosses * turn)[:, None], axis=0),
    ])
    first_weight = 1.0 / (1.0 + jnp.exp(route_logits[:, 1] - route_logits[:, 0]))
    second_weight = 1.0 / (1.0 + jnp.exp(route_logits[:, 0] - route_logits[:, 1]))
    coef = jnp.where(route_ids[:, 0:1] == expert_at[None, :], first_weight[:, None], 0.0)
    coef = coef + jnp.where(route_ids[:, 1:2] == expert_at[None, :], second_weight[:, None], 0.0)
    coef = jnp.pad(coef, ((0, 0), (0, LANES - n)))
    levels = sorted({max(1, half * eighths // 8) for eighths in (3, 4, 5, 6, 8)})
    crossing = jnp.sum(crosses) // 2
    level = sum((crossing > most).astype(jnp.int32) for most in levels[:-1])
    branches = [functools.partial(call_layer, n, most, i) for i, most in enumerate(levels)]
    return lax.switch(level, branches, table, tokens, coef, held_gate, held_up, held_down)


def solution(mesh):
    split = ("groups", "expert")
    placed = (
        P(split, None),
        P(split, None),
        P(split, None),
        P(),
        P(),
        P(split, None, None),
        P(split, None, None),
        P(split, None, None),
    )
    return jax.shard_map(
        per_device,
        mesh=mesh,
        in_specs=placed,
        out_specs=(
            P(split, None),
            P(split, None, None),
            P(split, None, None),
            P(split, None, None),
        ),
        check_vma=False,
    )
```

```python
import functools

import jax
import jax.numpy as jnp
from jax import lax
from jax.experimental import pallas as pl
from jax.experimental.pallas import tpu as pltpu
from jax.sharding import PartitionSpec as P

EXPERTS = 8
LANES = 128
MESH = pl.DeviceIdType.MESH
VMEM_BYTES = 63_000_000


def near_square_root(n):
    size = 1
    while size * size < n:
        size *= 2
    return size


def layer_kernel(
    n,
    most,
    table,
    tok,
    coef,
    held_g,
    held_u,
    held_d,
    out,
    moved_g,
    moved_u,
    moved_d,
    tok_all,
    coef_all,
    w_gu,
    w_d,
    pieces_g,
    pieces_u,
    pieces_d,
    crossed_g,
    crossed_u,
    crossed_d,
    ordered,
    hidden,
    contrib,
    part_in,
    plane_sum,
    half_in,
    cross_out,
    cross_in,
    load_sem,
    tok_send,
    fwd_send,
    plane_send,
    tok_recv,
    one_send,
    one_recv,
    two_send,
    two_recv,
    three_send,
    three_recv,
    part_send,
    part_recv,
    half_send,
    half_recv,
    cross_send,
    cross_recv,
):
    me = lax.axis_index("expert")
    half = n // 2
    base = (me // half) * half
    lane = me - base
    twin = lax.rem(me + half, n)
    rows, width = tok.shape
    band = width // half
    size = near_square_root(n)
    planes = n // size
    half_planes = planes // 2
    plane = me // size
    seat = me - plane * size
    my_plane_of_half = lane // size
    held = (held_g, held_u, held_d)
    moved = (moved_g, moved_u, moved_d)
    pieces = (pieces_g, pieces_u, pieces_d)
    crossed = (crossed_g, crossed_u, crossed_d)

    barrier = pltpu.get_barrier_semaphore()

    @pl.loop(1, n)
    def _(k):
        pl.semaphore_signal(
            barrier, inc=1, device_id={"expert": lax.rem(me + k, n)}, device_id_type=MESH
        )

    loads = (
        pltpu.make_async_copy(held_g.at[0], w_gu.at[:, pl.ds(0, LANES)], load_sem.at[0]),
        pltpu.make_async_copy(held_u.at[0], w_gu.at[:, pl.ds(LANES, LANES)], load_sem.at[1]),
        pltpu.make_async_copy(held_d.at[0], w_d, load_sem.at[2]),
    )
    for load in loads:
        load.start()

    def token_rows(owner):
        return pl.ds(pl.multiple_of(owner * rows, rows), rows)

    def band_rows(owner):
        return pl.ds(pl.multiple_of(owner * band, band), band)

    def near(k):
        return base + lax.rem(lane + k, half)

    def column(k):
        return base + lax.rem(lane + k * size, half)

    def mate(k):
        return plane * size + lax.rem(seat + k, size)

    def seated(other_plane):
        return other_plane * size + seat

    tok_all[token_rows(me), :] = tok[...]
    coef_all[token_rows(me), :] = coef[...]
    pl.semaphore_wait(barrier, n - 1)

    def send(source, target, send_sem, recv_sem, peer):
        return pltpu.make_async_remote_copy(
            src_ref=source, dst_ref=target, send_sem=send_sem, recv_sem=recv_sem,
            device_id={"expert": peer}, device_id_type=MESH,
        )

    def own_tokens(peer):
        at = token_rows(me)
        return (
            send(tok, tok_all.at[at], tok_send.at[0, peer], tok_recv.at[0, me], peer),
            send(coef, coef_all.at[at], tok_send.at[1, peer], tok_recv.at[1, me], peer),
        )

    def passed_tokens(owner, peer, sems):
        at = token_rows(owner)
        return (
            send(tok_all.at[at], tok_all.at[at], sems[0], tok_recv.at[0, owner], peer),
            send(coef_all.at[at], coef_all.at[at], sems[1], tok_recv.at[1, owner], peer),
        )

    def twin_tokens(peer):
        return passed_tokens(twin, peer, (fwd_send.at[0, peer], fwd_send.at[1, peer]))

    def plane_tokens(other_plane, k):
        sems = (plane_send.at[0, other_plane, k], plane_send.at[1, other_plane, k])
        return passed_tokens(seated(other_plane), mate(k), sems)

    def tokens_arrive(owner):
        pltpu.make_async_copy(tok, tok_all.at[token_rows(owner)], tok_recv.at[0, owner]).wait()
        pltpu.make_async_copy(coef, coef_all.at[token_rows(owner)], tok_recv.at[1, owner]).wait()

    def spread(array):
        pltpu.make_async_copy(
            held[array].at[0, band_rows(lane)], pieces[array].at[lane], one_recv.at[array]
        ).start()

        @pl.loop(1, half)
        def _(k):
            peer = near(k)
            send(
                held[array].at[0, band_rows(peer - base)], pieces[array].at[lane],
                one_send.at[array], one_recv.at[array], peer,
            ).start()

    def swap(array):
        return send(
            ordered.at[array, pl.ds(0, most)], crossed[array],
            two_send.at[array], two_recv.at[array], twin,
        )

    def cross_over(array):
        pltpu.make_async_copy(pieces[array], pieces[array], one_recv.at[array]).wait()

        @pl.loop(0, most)
        def _(m):
            ordered[array, m] = pieces[array][table[base + m]]

        swap(array).start()

    def deliver(array):
        swap(array).wait()

        @pl.loop(0, half)
        def _(place):
            at = base + place
            own = pieces[array][table[2 * n + at]]
            other = crossed[array][table[3 * n + at]]
            ordered[array, place] = jnp.where(table[n + at] == 1, other, own)

        pltpu.make_async_copy(
            ordered.at[array, lane], moved[array].at[0, band_rows(lane)], three_recv.at[array]
        ).start()

        @pl.loop(1, half)
        def _(k):
            peer = near(k)
            send(
                ordered.at[array, peer - base], moved[array].at[0, band_rows(lane)],
                three_send.at[array], three_recv.at[array], peer,
            ).start()

    for copy in own_tokens(twin):
        copy.start()

    @pl.loop(1, half_planes)
    def _(k):
        for copy in own_tokens(column(k)):
            copy.start()

    @pl.loop(1, size)
    def _(k):
        for copy in own_tokens(mate(k)):
            copy.start()

    spread(0)
    tokens_arrive(twin)

    @pl.loop(1, half_planes)
    def _(k):
        for copy in twin_tokens(column(k)):
            copy.start()

    spread(1)

    @pl.loop(1, half_planes)
    def _(k):
        tokens_arrive(column(k))
        tokens_arrive(lax.rem(column(k) + half, n))

    @pl.loop(1, planes)
    def _(shift):
        @pl.loop(1, size)
        def _(k):
            for copy in plane_tokens(lax.rem(plane + shift, planes), k):
                copy.start()

    spread(2)
    cross_over(0)
    cross_over(1)

    @pl.loop(0, planes)
    def _(other_plane):
        @pl.loop(1, size)
        def _(k):
            tokens_arrive(other_plane * size + lax.rem(seat + k, size))

    for load in loads:
        load.wait()

    step = min(256, n * rows)
    columns = 512

    @pl.loop(0, n * rows // step)
    def _(block):
        at = pl.ds(pl.multiple_of(block * step, step), step)
        both = jnp.dot(tok_all[at, :], w_gu[...], preferred_element_type=jnp.float32)
        gate_value = both[:, :LANES]
        up_value = both[:, LANES:]
        hidden[...] = (gate_value / (1.0 + jnp.exp(-gate_value)) * up_value).astype(jnp.bfloat16)
        lanes = lax.broadcasted_iota(jnp.int32, (step, LANES), 1)
        scale = jnp.sum(jnp.where(lanes == me, coef_all[at, :], 0.0), axis=1, keepdims=True)

        @pl.loop(0, width // columns)
        def _(part):
            cols = pl.ds(pl.multiple_of(part * columns, columns), columns)
            value = lax.dot_general(
                hidden[...], w_d[cols, :], (((1,), (1,)), ((), ())),
                preferred_element_type=jnp.float32,
            )
            value = value.astype(jnp.bfloat16).astype(jnp.float32)
            contrib[at, cols] = (value * scale).astype(jnp.bfloat16)

    def part_copy(k, other_plane):
        peer = mate(k)
        owner = other_plane * size + lax.rem(seat + k, size)
        return send(
            contrib.at[token_rows(owner)], part_in.at[seat, other_plane],
            part_send.at[k, other_plane], part_recv.at[seat, other_plane], peer,
        )

    def half_copy(k, kind):
        peer = column(k)
        target = peer // size if kind == 0 else lax.rem(peer // size + half_planes, planes)
        return send(
            plane_sum.at[target], half_in.at[kind, my_plane_of_half],
            half_send.at[kind, k], half_recv.at[kind, my_plane_of_half], peer,
        )

    @pl.loop(0, planes)
    def _(other_plane):
        @pl.loop(1, size)
        def _(k):
            part_copy(k, other_plane).start()

    def add_plane():
        @pl.loop(0, planes)
        def _(other_plane):
            @pl.loop(1, size)
            def _(k):
                spot = part_in.at[lax.rem(seat + k, size), other_plane]
                pltpu.make_async_copy(
                    spot, spot, part_recv.at[lax.rem(seat + k, size), other_plane]
                ).wait()

            @pl.loop(0, width // columns)
            def _(part):
                cols = pl.ds(pl.multiple_of(part * columns, columns), columns)

                def more(k, total):
                    other = lax.rem(seat + k, size)
                    return total + part_in[other, other_plane, :, cols].astype(jnp.float32)

                total = contrib[token_rows(seated(other_plane)), cols].astype(jnp.float32)
                total = lax.fori_loop(1, size, more, total)
                plane_sum[other_plane, :, cols] = total.astype(jnp.bfloat16)

        for kind in (1, 0):

            @pl.loop(1, half_planes)
            def _(k):
                half_copy(k, kind).start()

    def add_half(kind, own_plane, extra, target):
        @pl.loop(1, half_planes)
        def _(k):
            other = lax.rem(my_plane_of_half + k, half_planes)
            spot = half_in.at[kind, other]
            pltpu.make_async_copy(spot, spot, half_recv.at[kind, other]).wait()

        @pl.loop(0, width // columns)
        def _(part):
            cols = pl.ds(pl.multiple_of(part * columns, columns), columns)

            def more(k, total):
                other = lax.rem(my_plane_of_half + k, half_planes)
                return total + half_in[kind, other, :, cols].astype(jnp.float32)

            total = plane_sum[own_plane, :, cols].astype(jnp.float32)
            if extra is not None:
                total = total + extra[:, cols].astype(jnp.float32)
            target[:, cols] = lax.fori_loop(1, half_planes, more, total).astype(jnp.bfloat16)

    deliver(0)
    cross_over(2)
    add_plane()
    deliver(1)
    add_half(1, lax.rem(plane + half_planes, planes), None, cross_out)
    cross = send(cross_out, cross_in, cross_send, cross_recv, twin)
    cross.start()
    deliver(2)
    cross.wait()
    add_half(0, plane, cross_in, out)

    for copy in own_tokens(twin):
        copy.wait_send()

    @pl.loop(1, half_planes)
    def _(k):
        for copy in own_tokens(column(k)):
            copy.wait_send()
        for copy in twin_tokens(column(k)):
            copy.wait_send()
        half_copy(k, 0).wait_send()
        half_copy(k, 1).wait_send()

    @pl.loop(1, size)
    def _(k):
        for copy in own_tokens(mate(k)):
            copy.wait_send()

        @pl.loop(0, planes)
        def _(other_plane):
            part_copy(k, other_plane).wait_send()

        @pl.loop(1, planes)
        def _(shift):
            for copy in plane_tokens(lax.rem(plane + shift, planes), k):
                copy.wait_send()

    for array in range(3):
        sent = pieces[array].at[pl.ds(0, half - 1)]
        pltpu.make_async_copy(sent, sent, one_send.at[array]).wait()
        pltpu.make_async_copy(sent, sent, three_send.at[array]).wait()
        pltpu.make_async_copy(
            moved[array].at[0], moved[array].at[0], three_recv.at[array]
        ).wait()


def call_layer(n, most, which, table, tokens, coef, held_gate, held_up, held_down):
    rows, width = tokens.shape
    half = n // 2
    band = width // half
    size = near_square_root(n)
    planes = n // size
    vmem = pl.BlockSpec(memory_space=pltpu.VMEM)
    anywhere = pl.BlockSpec(memory_space=pl.ANY)
    dma = pltpu.SemaphoreType.DMA
    moved_shape = jax.ShapeDtypeStruct(held_gate.shape, held_gate.dtype)

    def block(*shape):
        return pltpu.VMEM(shape, jnp.bfloat16)

    return pl.pallas_call(
        functools.partial(layer_kernel, n, most),
        out_shape=(jax.ShapeDtypeStruct((rows, width), jnp.bfloat16),) + (moved_shape,) * 3,
        in_specs=[pl.BlockSpec(memory_space=pltpu.SMEM), vmem, vmem] + [anywhere] * 3,
        out_specs=(vmem, anywhere, anywhere, anywhere),
        scratch_shapes=[
            block(n * rows, width),
            pltpu.VMEM((n * rows, LANES), jnp.float32),
            block(width, 2 * LANES),
            block(width, LANES),
            block(half, band, LANES),
            block(half, band, LANES),
            block(half, band, LANES),
            block(most, band, LANES),
            block(most, band, LANES),
            block(most, band, LANES),
            block(3, half, band, LANES),
            block(min(256, n * rows), LANES),
            block(n * rows, width),
            block(size, planes, rows, width),
            block(planes, rows, width),
            block(2, planes // 2, rows, width),
            block(rows, width),
            block(rows, width),
            dma((3,)),
            dma((2, n)),
            dma((2, n)),
            dma((2, planes, size)),
            dma((2, n)),
            dma((3,)),
            dma((3,)),
            dma((3,)),
            dma((3,)),
            dma((3,)),
            dma((3,)),
            dma((size, planes)),
            dma((size, planes)),
            dma((2, planes // 2)),
            dma((2, planes // 2)),
            dma,
            dma,
        ],
        compiler_params=pltpu.CompilerParams(
            collective_id=which, has_side_effects=True, vmem_limit_bytes=VMEM_BYTES
        ),
    )(table, tokens, coef, held_gate, held_up, held_down)


def per_device(
    tokens, route_ids, route_logits, old_place, new_place, held_gate, held_up, held_down
):
    n = lax.axis_size("expert")
    half = n // 2
    device_ids = jnp.arange(n, dtype=jnp.int32)
    blocks = n // EXPERTS
    at_old = (old_place[:, None] == device_ids[None, :]).astype(jnp.int32)
    dest_of = jnp.sum(at_old * new_place[:, None], axis=0)
    expert_at = jnp.sum(at_old * device_ids[:, None], axis=0) // blocks
    half_of = device_ids // half
    crosses = (dest_of // half != half_of).astype(jnp.int32)
    earlier = (half_of[:, None] == half_of[None, :]) & (device_ids[:, None] < device_ids[None, :])
    turn = jnp.sum(earlier.astype(jnp.int32) * crosses[:, None], axis=0)
    lane_of = device_ids - half_of * half
    leaving = (half_of[:, None] * half + turn[:, None] == device_ids[None, :]).astype(jnp.int32)
    leaving = jnp.sum(leaving * (crosses * lane_of)[:, None], axis=0)
    arriving = (dest_of[:, None] == device_ids[None, :]).astype(jnp.int32)
    table = jnp.concatenate([
        leaving,
        jnp.sum(arriving * crosses[:, None], axis=0),
        jnp.sum(arriving * ((1 - crosses) * lane_of)[:, None], axis=0),
        jnp.sum(arriving * (crosses * turn)[:, None], axis=0),
    ])
    first_weight = 1.0 / (1.0 + jnp.exp(route_logits[:, 1] - route_logits[:, 0]))
    second_weight = 1.0 / (1.0 + jnp.exp(route_logits[:, 0] - route_logits[:, 1]))
    coef = jnp.where(route_ids[:, 0:1] == expert_at[None, :], first_weight[:, None], 0.0)
    coef = coef + jnp.where(route_ids[:, 1:2] == expert_at[None, :], second_weight[:, None], 0.0)
    coef = jnp.pad(coef, ((0, 0), (0, LANES - n)))
    table, coef = lax.optimization_barrier((table, coef))
    levels = sorted({max(1, half * eighths // 8) for eighths in (3, 4, 5, 6, 8)})
    crossing = jnp.sum(crosses) // 2
    level = sum((crossing > most).astype(jnp.int32) for most in levels[:-1])
    branches = [functools.partial(call_layer, n, most, i) for i, most in enumerate(levels)]
    return lax.switch(level, branches, table, tokens, coef, held_gate, held_up, held_down)


def solution(mesh):
    split = ("groups", "expert")
    placed = (
        P(split, None),
        P(split, None),
        P(split, None),
        P(),
        P(),
        P(split, None, None),
        P(split, None, None),
        P(split, None, None),
    )
    return jax.shard_map(
        per_device,
        mesh=mesh,
        in_specs=placed,
        out_specs=(
            P(split, None),
            P(split, None, None),
            P(split, None, None),
            P(split, None, None),
        ),
        check_vma=False,
    )
```
